32 devices in a mesh: gx: 2 (over y), gy: 4 (over x, core), gz: 4 (over z).
Axes of the slice: x: 2, y: 2, z: 4, core: 2. Of those that a mesh axis runs over, the one named last changes fastest.
Arguments:
- pressure: float32 [24, 64, 512], P('gx', 'gy', 'gz'), may hold values from -8 to 8
- wind: float32 [3, 24, 64, 512], P(None, 'gx', 'gy', 'gz'), may hold values from -6 to 6
Outputs:
- result: float32 [24, 64, 512], P('gx', 'gy', 'gz')
The draws below stay inside these ranges and needn't reach their ends.
All inputs are finite; a program needn't handle non-finite values.
Results may differ from the reference program's by a relative error of at most 0.00019.
Values sent between devices are 32-bit elements; how exact they have to be, the bound alone decides.
A program may use at most 64 MiB of HBM per device.

```python
import jax
import jax.numpy as jnp

SWEEPS = 2
COARSE_SWEEPS = 4
CYCLES = 1
NX = 24
NY = 64
NZ = 512


def draw_pressure(key, part):
    noise = jax.random.normal(key, (NX, NY, NZ), jnp.float32)
    return jnp.clip(noise, -8.0, 8.0)


def level_of(own_key, dims, split, low, high):
    factor_of = 1.0
    for dim, blocks in split:
        draws = jax.random.uniform(jax.random.fold_in(jax.random.fold_in(own_key, 6), dim), (blocks,), jnp.float32, low / len(split), high / len(split))
        factor_of = factor_of * jnp.repeat(jnp.exp(draws), dims[dim] // blocks).reshape((-1,) + (1,) * (len(dims) - 1 - dim))
    return factor_of


def normal_values(key, shape, deviation, limit, shards=(), held_as=jnp.bfloat16):
    array = jax.random.normal(key, shape, jnp.float32) * deviation
    if len(shards) > 0:
        array = level_of(key, shape, shards, -0.22, 0.18) * array
    return jnp.clip(array, min=-limit, max=limit).astype(held_as)


def setup_inputs(seed: int = 0) -> dict:
    keys = jax.random.split(jax.random.key(seed), 3)
    pressure = draw_pressure(jax.random.fold_in(keys[2], 71), 0)
    wind = normal_values(keys[1], (3, NX, NY, NZ), 1.0, 6.0, ((1, 2), (2, 4), (3, 4)), jnp.float32)
    return {"pressure": pressure, "wind": wind}


OMEGA = 0.8
VISCOSITY = 1.0
REACTION = 1.0


def six_sum(padded):
    return (padded[..., 2:, 1:-1, 1:-1] + padded[..., :-2, 1:-1, 1:-1]
            + padded[..., 1:-1, 2:, 1:-1] + padded[..., 1:-1, :-2, 1:-1]
            + padded[..., 1:-1, 1:-1, 2:] + padded[..., 1:-1, 1:-1, :-2])


def central_parts(padded):
    return ((padded[..., 2:, 1:-1, 1:-1] - padded[..., :-2, 1:-1, 1:-1]) * 0.5,
            (padded[..., 1:-1, 2:, 1:-1] - padded[..., 1:-1, :-2, 1:-1]) * 0.5,
            (padded[..., 1:-1, 1:-1, 2:] - padded[..., 1:-1, 1:-1, :-2]) * 0.5)


def pad_space(values):
    return jnp.pad(values, [(0, 0)] * (values.ndim - 3) + [(1, 1), (1, 1), (1, 1)])


def laplace(values, padded, weight_scale):
    return weight_scale * (6.0 * values - six_sum(padded))


def sweep(source, values, padded, weight_scale):
    return values + (OMEGA / (6.0 * weight_scale)) * (source - laplace(values, padded, weight_scale))


def start_sweep(source, weight_scale):
    return (OMEGA / (6.0 * weight_scale)) * source


def smooth(source, values, weight_scale, sweep_count):
    for sweep_number in range(sweep_count):
        if values is None:
            values = start_sweep(source, weight_scale)
        else:
            values = sweep(source, values, pad_space(values), weight_scale)
    return values


def restrict(values):
    extent_x, extent_y, extent_z = values.shape
    blocks = values.reshape(extent_x // 2, 2, extent_y // 2, 2, extent_z // 2, 2)
    return 0.125 * jnp.sum(blocks, axis=(1, 3, 5))


def prolong(values):
    extent_x, extent_y, extent_z = values.shape
    spread = jnp.broadcast_to(values[:, None, :, None, :, None], (extent_x, 2, extent_y, 2, extent_z, 2))
    return spread.reshape(2 * extent_x, 2 * extent_y, 2 * extent_z)


def vcycle(source, values, depth_index):
    weight_scale = 0.25 ** depth_index
    if depth_index == 2:
        return smooth(source, None, weight_scale, COARSE_SWEEPS)
    values = smooth(source, values, weight_scale, SWEEPS)
    residual = source - laplace(values, pad_space(values), weight_scale)
    correction = vcycle(restrict(residual), None, depth_index + 1)
    values = values + prolong(correction)
    return smooth(source, values, weight_scale, SWEEPS)


def solve(source):
    values = None
    for cycle_number in range(CYCLES):
        values = vcycle(source, values, 0)
    return values


def momentum(padded_velocity, wind):
    centre = padded_velocity[:, 1:-1, 1:-1, 1:-1]
    diffusion = 6.0 * centre - six_sum(padded_velocity)
    slopes = central_parts(padded_velocity)
    convection = wind[0:1] * slopes[0] + wind[1:2] * slopes[1] + wind[2:3] * slopes[2]
    return REACTION * centre + VISCOSITY * diffusion + convection


def reference(pressure, wind):
    first = solve(pressure)
    velocity = jnp.stack(central_parts(pad_space(first)))
    flux = momentum(pad_space(velocity), wind)
    slopes = central_parts(pad_space(flux))
    product = -(slopes[0][0] + slopes[1][1] + slopes[2][2])
    return solve(product)
```

```python
import functools

import jax
import jax.numpy as jnp
from jax import lax
from jax.experimental import pallas as pl
from jax.experimental.pallas import tpu as pltpu
from jax.sharding import PartitionSpec as P

MESH = pl.DeviceIdType.MESH
OMEGA = 0.8
KEEP = 1.0 - OMEGA
CS = OMEGA / 6.0
H = 8
HW = 3
ZS = 8
L1S = 16
UNROLL = 2


def loop(low, high, step, unroll=UNROLL):
    def run(p, carry):
        step(p)
        return carry

    lax.fori_loop(low, high, run, 0, unroll=min(unroll, high - low))


def kernel(
    counts, local,
    p_ref, w_ref, o_ref,
    pr, va, vb, vel, flux, wr, m2, bz, wzr, pk, wpk,
    s16, cat, b1, v1, r1, b2, u2, e1, tmp, ex, tall,
    m1s, m2s, m1r, m2r, fs, fr,
    psend, precv, wsend, wrecv, gsend, grecv, fsend, frecv,
):
    gx, gy, gz = counts
    nx, ny, nz = local
    cx, cy, cz = nx // 2, ny // 2, nz // 2
    mx, my, mz = lax.axis_index("gx"), lax.axis_index("gy"), lax.axis_index("gz")
    me = mx * gy + my
    group = gx * gy

    def exists(dx, dy, dz):
        ok = None
        for d, m, g in ((dx, mx, gx), (dy, my, gy), (dz, mz, gz)):
            if d:
                here = (m + d >= 0) & (m + d < g)
                ok = here if ok is None else ok & here
        return ok

    barrier = pltpu.get_barrier_semaphore()

    def peers(act):
        def at(t):
            ax, ay = t // gy, t % gy
            for dz in (-1, 0, 1):
                ok = (mz + dz >= 0) & (mz + dz < gz)
                if dz == 0:
                    ok = t != me

                @pl.when(ok)
                def _():
                    act(t, ax, ay, dz)

        loop(0, group, at, 1)

    peers(lambda t, ax, ay, dz: pl.semaphore_signal(
        barrier, inc=1, device_id=(ax, ay, mz + dz), device_id_type=MESH))

    row = lax.broadcasted_iota(jnp.int32, (ny + 2 * H, 2 * nz), 0) - H
    lane = lax.broadcasted_iota(jnp.int32, (ny + 2 * H, 2 * nz), 1)
    zpos = jnp.where(lane < nz + nz // 2, lane, lane - 2 * nz)
    inside = (
        (row + my * ny >= 0) & (row + my * ny < gy * ny)
        & (zpos + mz * nz >= 0) & (zpos + mz * nz < gz * nz)
    )
    m2[...] = inside.astype(jnp.float32)

    def sx(p):
        x = mx * nx + p - H
        return jnp.where((x >= 0) & (x < gx * nx), 1.0, 0.0).astype(jnp.float32)

    lane1 = lax.broadcasted_iota(jnp.int32, (ny, nz), 1)
    lo, hi = jnp.zeros((ny, nz), jnp.float32), jnp.zeros((ny, nz), jnp.float32)
    for i in range(nx):
        plane = p_ref[i]
        a = plane if i == 0 else pltpu.roll(plane, ZS * i, 1)
        b = pltpu.roll(plane, (ZS * (i + 1)) % nz, 1)
        sel = (lane1 >= ZS * i) & (lane1 < ZS * (i + 1))
        lo = jnp.where(sel, a, lo)
        hi = jnp.where(sel, b, hi)
    pk[0] = lo
    pk[1] = hi
    lo, hi = jnp.zeros((ny, nz), jnp.float32), jnp.zeros((ny, nz), jnp.float32)
    for e in range(3):
        for i in range(nx):
            at = HW * (e * nx + i)
            plane = w_ref[e, i]
            a = plane if at == 0 else pltpu.roll(plane, at, 1)
            b = pltpu.roll(plane, (at + HW) % nz, 1)
            sel = (lane1 >= at) & (lane1 < at + HW)
            lo = jnp.where(sel, a, lo)
            hi = jnp.where(sel, b, hi)
    wpk[0] = lo
    wpk[1] = hi

    n_peers = 3 * group - 1
    n_peers = n_peers - jnp.where(mz == 0, group, 0) - jnp.where(mz == gz - 1, group, 0)
    pl.semaphore_wait(barrier, n_peers)

    def span(d, n, h, big):
        if d == 0:
            return pl.ds(0, n), pl.ds(big, n)
        if d > 0:
            return pl.ds(n - h, h), pl.ds(0, h)
        return pl.ds(0, h), pl.ds(big + n, h)

    offsets = [
        (dx, dy, dz) for dz in (0, -1, 1) for dx in (0, -1, 1) for dy in (0, -1, 1)
        if (dx, dy, dz) != (0, 0, 0)
        and (gx > 1 or dx == 0) and (gy > 1 or dy == 0) and (gz > 1 or dz == 0)
    ]

    def key(d):
        return (d[0] + 1) * 9 + (d[1] + 1) * 3 + d[2] + 1

    def pcopy(d):
        dx, dy, dz = d
        to = (mx + dx, my + dy, mz + dz)
        k = key(d)
        if dz == 0:
            xs, xd = span(dx, nx, H, H)
            ys, yd = span(dy, ny, H, H)
            src, dst = p_ref.at[xs, ys], pr.at[xd, yd, pl.ds(0, nz)]
        else:
            src = pk.at[0 if dz < 0 else 1]
            dst = bz.at[0 if dz < 0 else 1, (1 - dx) * 3 + 1 - dy]
        return pltpu.make_async_remote_copy(
            src_ref=src, dst_ref=dst, send_sem=psend.at[k], recv_sem=precv.at[k],
            device_id=to, device_id_type=MESH)

    def wcopy(d):
        dx, dy, dz = d
        to = (mx + dx, my + dy, mz + dz)
        k = key(d)
        if dz == 0:
            xs, xd = span(dx, nx, HW, HW)
            ys, yd = span(dy, ny, H, H)
            src, dst = w_ref.at[:, xs, ys], wr.at[:, xd, yd, pl.ds(0, nz)]
        else:
            src = wpk.at[0 if dz < 0 else 1]
            dst = wzr.at[0 if dz < 0 else 1, (1 - dx) * 3 + 1 - dy]
        return pltpu.make_async_remote_copy(
            src_ref=src, dst_ref=dst, send_sem=wsend.at[k], recv_sem=wrecv.at[k],
            device_id=to, device_id_type=MESH)

    def opposite(d):
        return (-d[0], -d[1], -d[2])

    for d in offsets:
        pl.when(exists(*d))(lambda d=d: pcopy(d).start())
    for d in offsets:
        pl.when(exists(*d))(lambda d=d: wcopy(d).start())

    pr[H : H + nx, H : H + ny, 0:nz] = p_ref[...]
    wr[:, HW : HW + nx, H : H + ny, 0:nz] = w_ref[...]

    for d in offsets:
        pl.when(exists(*opposite(d)))(lambda d=d: pcopy(d).wait_recv())

    lane_h = lax.broadcasted_iota(jnp.int32, (ny + 2 * H, nz), 1)

    def rows_of(buf, side, ix, comp=None):
        parts = []
        for iy, (s, n) in enumerate(((ny - H, H), (0, ny), (0, H))):
            parts.append(buf[side, ix * 3 + iy, pl.ds(s, n), :])
        return jnp.concatenate(parts, axis=0)

    def clean(buf_lo, buf_hi, at, width):
        right = buf_lo if at == 0 else pltpu.roll(buf_lo, nz - at, 1)
        left = pltpu.roll(buf_hi, (2 * nz - width - at) % nz, 1)
        return jnp.where(lane_h < width, right, jnp.where(lane_h >= nz - width, left, 0.0))

    okmask = m2[...] > 0.5
    for ix, (first, low, n) in enumerate(((nx - H, 0, H), (0, H, nx), (0, H + nx, H))):
        right, left = rows_of(bz, 0, ix), rows_of(bz, 1, ix)
        for i in range(n):
            p = low + i
            halo = clean(right, left, ZS * (first + i), ZS)
            x = mx * nx + p - H
            good = okmask & ((x >= 0) & (x < gx * nx))
            pr[p, :, 0:nz] = jnp.where(good[:, :nz], pr[p, :, 0:nz], 0.0)
            pr[p, :, nz:] = jnp.where(good[:, nz:], halo, 0.0)

    ry, rz = ny + 2 * H, 2 * nz

    def up(v, axis, k=1):
        return pltpu.roll(v, v.shape[axis] - k, axis)

    def down(v, axis, k=1):
        return pltpu.roll(v, k, axis)

    def six(ref, p, centre):
        return (
            (ref[p + 1] + ref[p - 1])
            + (up(centre, 0) + down(centre, 0))
            + (up(centre, 1) + down(centre, 1))
        )

    CB0 = OMEGA / 6.0

    def pre(src, dst, low, high):
        def at(p):
            c = src[p]
            dst[p] = (CB0 * (1.2 * c + CS * six(src, p, c))) * (sx(p) * m2[...])

        loop(low, high, at)

    li = lax.broadcasted_iota(jnp.int32, (nz, nz), 0)
    lj = lax.broadcasted_iota(jnp.int32, (nz, nz), 1)
    squeeze = jnp.where(li // 2 == lj % cz, 0.125, 0.0).astype(jnp.float32)
    ei = lax.broadcasted_iota(jnp.int32, (nz, 2 * nz), 0)
    ej = lax.broadcasted_iota(jnp.int32, (nz, 2 * nz), 1)
    spread = jnp.where(ej // 2 == ei, 1.0, 0.0).astype(jnp.float32)

    lane8 = lax.broadcasted_iota(jnp.int32, (cy, nz), 1)
    z1 = jnp.where(lane8 < nz - cz // 2, lane8, lane8 - nz)
    zin1 = (
        (z1 + mz * cz >= 0) & (z1 + mz * cz < gz * cz)
        & (z1 >= -L1S) & (z1 < cz + L1S)
    )
    tr = 8 + gy * cy
    row1 = lax.broadcasted_iota(jnp.int32, (tr, nz), 0)
    lan1 = lax.broadcasted_iota(jnp.int32, (tr, nz), 1)
    zl1 = jnp.where(lan1 < nz - cz // 2, lan1, lan1 - nz)
    mask1 = (
        (row1 >= 4) & (row1 < tr - 4)
        & (zl1 + mz * cz >= 0) & (zl1 + mz * cz < gz * cz)
    ).astype(jnp.float32)
    hy = gy * cy // 2
    row2 = lax.broadcasted_iota(jnp.int32, (hy, nz), 0)
    lan2 = lax.broadcasted_iota(jnp.int32, (hy, nz), 1)
    zl2 = jnp.where(lan2 < nz - cz // 2, lan2, lan2 - nz)
    mask2 = ((zl2 + mz * cz >= 0) & (zl2 + mz * cz < gz * cz)).astype(jnp.float32)
    not_first = (row2 > 0).astype(jnp.float32)
    not_last = (row2 < hy - 1).astype(jnp.float32)
    even2 = lan2 % 2 == 0

    X1 = gx * cx
    X2 = X1 // 2
    zero1 = jnp.zeros((tr, nz), jnp.float32)
    zero2 = jnp.zeros((hy, nz), jnp.float32)
    for ref in (b1, v1, r1, e1):
        ref[0] = zero1
        ref[X1 + 1] = zero1
    loop(1, X1 + 1, lambda p: b1.__setitem__(p, zero1))
    u2[0, 0] = zero2
    u2[0, X2 + 1] = zero2
    u2[1, 0] = zero2
    u2[1, X2 + 1] = zero2

    def gcopy(turn, t, ax, ay, dz, slot):
        side = dz + 1
        if dz == 0:
            src, dst = m1s.at[turn], m1r.at[turn, slot]
        else:
            src = m2s.at[turn, 0 if dz < 0 else 1]
            dst = m2r.at[turn, slot, 0 if dz < 0 else 1]
        return pltpu.make_async_remote_copy(
            src_ref=src, dst_ref=dst, send_sem=gsend.at[turn, t, side],
            recv_sem=grecv.at[turn, slot, side],
            device_id=(ax, ay, mz + dz), device_id_type=MESH)

    def coarse_source(turn, src, v):
        for i in range(cx):
            parts = []
            for q in (H + 2 * i, H + 2 * i + 1):
                c = v[q]
                r = src[q] - 6.0 * c + six(v, q, c)
                parts.append(r[H : H + ny, 0:nz])
            s16[i] = parts[0] + parts[1]
            cat[cy * i : cy * (i + 1)] = (
                s16[i, pl.ds(0, cy, stride=2), :] + s16[i, pl.ds(1, cy, stride=2), :]
            )
        c1 = lax.dot_general(
            cat[...], squeeze, (((1,), (0,)), ((), ())),
            precision=lax.Precision.HIGHEST, preferred_element_type=jnp.float32)
        planes = [c1[cy * i : cy * (i + 1)] for i in range(cx)]
        for i in range(cx // 2):
            m1s[turn, i] = jnp.where(lane8 < cz, planes[i], planes[i + cx // 2])
            m1r[turn, me, i] = jnp.where(lane8 < cz, planes[i], planes[i + cx // 2])
        lo = jnp.zeros((cy, nz), jnp.float32)
        hi = jnp.zeros((cy, nz), jnp.float32)
        for i in range(cx):
            sel = (lane8 >= L1S * i) & (lane8 < L1S * (i + 1))
            a = planes[i] if i == 0 else pltpu.roll(planes[i], L1S * i, 1)
            b = pltpu.roll(planes[i], (L1S * i + nz - cz + L1S) % nz, 1)
            lo = jnp.where(sel, a, lo)
            hi = jnp.where(sel, b, hi)
        m2s[turn, 0] = lo
        m2s[turn, 1] = hi
        peers(lambda t, ax, ay, dz: gcopy(turn, t, ax, ay, dz, me).start())

    def coarse_gather(turn):
        def at(t):
            ax, ay = t // gy, t % gy
            for dz in (-1, 0, 1):
                ok = (mz - dz >= 0) & (mz - dz < gz)
                if dz == 0:
                    ok = t != me

                @pl.when(ok)
                def _():
                    gcopy(turn, t, ax, ay, dz, t).wait_recv()

        loop(0, group, at, 1)
        for t in range(group):
            ax, ay = t // gy, t % gy
            for i in range(cx):
                body = m1r[turn, t, i % (cx // 2)]
                if i >= cx // 2:
                    body = pltpu.roll(body, cz, 1)
                right = pltpu.roll(m2r[turn, t, 0], (cz - L1S * i) % nz, 1)
                left = pltpu.roll(m2r[turn, t, 1], (2 * nz - L1S - L1S * i) % nz, 1)
                whole = jnp.where(lane8 < cz, body, jnp.where(lane8 < nz - L1S, right, left))
                b1[1 + ax * cx + i, 4 + cy * ay : 4 + cy * (ay + 1)] = jnp.where(zin1, whole, 0.0)

    def coarse(turn):
        cb1 = OMEGA / (6.0 * 0.25)
        cb2 = OMEGA / (6.0 * 0.0625)

        def at(p):
            c = b1[p]
            v1[p] = (cb1 * (1.2 * c + CS * six(b1, p, c))) * mask1

        loop(1, X1 + 1, at)

        def residual(p):
            c = v1[p]
            return b1[p] - 0.25 * (6.0 * c - six(v1, p, c))

        def down_to_2(j):
            tall[...] = residual(2 * j + 1) + residual(2 * j + 2)
            s = tall[pl.ds(4, hy, stride=2), :] + tall[pl.ds(5, hy, stride=2), :]
            s = s + jnp.where(even2, up(s, 1), down(s, 1))
            s = (0.125 * s) * mask2
            b2[j + 1] = s
            u2[0, j + 1] = cb2 * s

        loop(0, X2, down_to_2)
        for number in range(3):
            a, b = number % 2, (number + 1) % 2

            def sweep2(j, a=a, b=b):
                c = u2[a, j]
                s = (
                    (u2[a, j + 1] + u2[a, j - 1])
                    + (up(c, 0) * not_last + down(c, 0) * not_first)
                    + (up(c, 1, 2) + down(c, 1, 2))
                )
                u2[b, j] = (KEEP * c + cb2 * b2[j] + CS * s) * mask2

            loop(1, X2 + 1, sweep2)

        tall[...] = zero1

        def up_to_1(j):
            e = u2[1, j + 1]
            tall[pl.ds(4, hy, stride=2), :] = e
            tall[pl.ds(5, hy, stride=2), :] = e
            t = tall[...]
            v1[2 * j + 1] = v1[2 * j + 1] + t
            v1[2 * j + 2] = v1[2 * j + 2] + t

        loop(0, X2, up_to_1)
        for src, dst in ((v1, r1), (r1, e1)):
            def sweep1(p, src=src, dst=dst):
                c = src[p]
                dst[p] = (KEEP * c + cb1 * b1[p] + CS * six(src, p, c)) * mask1

            loop(1, X1 + 1, sweep1)

    half = ry // 2

    def correct(v, low, high):
        first = low // 2
        last = (high + 1) // 2
        n = last - first
        for k in range(n):
            x = mx * cx + first + k - H // 2
            x = jnp.clip(x, 0, X1 - 1) + 1
            ex[half * k : half * (k + 1)] = e1[x, pl.ds(pl.multiple_of(my * cy, 8), half), :]
        wide = lax.dot_general(
            ex[0 : half * n], spread, (((1,), (0,)), ((), ())),
            precision=lax.Precision.HIGHEST, preferred_element_type=jnp.float32)
        m = m2[...]
        for k in range(n):
            piece = wide[half * k : half * (k + 1)]
            for h in range(2):
                tmp[k, h, pl.ds(0, half, stride=2), :] = piece[:, h * nz : (h + 1) * nz]
                tmp[k, h, pl.ds(1, half, stride=2), :] = piece[:, h * nz : (h + 1) * nz]
            for q in (2 * (first + k), 2 * (first + k) + 1):
                if low <= q < high:
                    for h in range(2):
                        ls = slice(h * nz, (h + 1) * nz)
                        v[q, :, ls] = v[q, :, ls] + tmp[k, h] * (sx(q) * m[:, ls])

    def post(b, src, dst, low, high):
        def at(p):
            c = src[p]
            dst[p] = (KEEP * c + CB0 * b[p] + CS * six(src, p, c)) * (sx(p) * m2[...])

        loop(low, high, at)

    pre(pr, va, 1, nx + 2 * H - 1)
    coarse_source(0, pr, va)
    coarse_gather(0)
    coarse(0)
    correct(va, 1, nx + 2 * H - 1)
    post(pr, va, vb, 2, nx + 2 * H - 2)
    post(pr, vb, va, 3, nx + 2 * H - 3)

    def velocity(p):
        c = va[p]
        m = (0.5 * sx(p)) * m2[...]
        vel[0, p] = (va[p + 1] - va[p - 1]) * m
        vel[1, p] = (up(c, 0) - down(c, 0)) * m
        vel[2, p] = (up(c, 1) - down(c, 1)) * m

    loop(4, nx + 2 * H - 4, velocity)

    for d in offsets:
        pl.when(exists(*opposite(d)))(lambda d=d: wcopy(d).wait_recv())
    for ix, (first, low, n) in enumerate(((nx - HW, 0, HW), (0, HW, nx), (0, HW + nx, HW))):
        right, left = rows_of(wzr, 0, ix), rows_of(wzr, 1, ix)
        for e in range(3):
            for i in range(n):
                p = low + i
                halo = clean(right, left, HW * (e * nx + first + i), HW)
                x = mx * nx + p - HW
                good = okmask & ((x >= 0) & (x < gx * nx))
                wr[e, p, :, 0:nz] = jnp.where(good[:, :nz], wr[e, p, :, 0:nz], 0.0)
                wr[e, p, :, nz:] = jnp.where(good[:, nz:], halo, 0.0)

    def momentum(p):
        m = sx(p) * m2[...]
        q = p - (H - HW)
        w0, w1, w2 = 0.5 * wr[0, q], 0.5 * wr[1, q], 0.5 * wr[2, q]
        for d in range(3):
            c, n, s = vel[d, p], vel[d, p + 1], vel[d, p - 1]
            yu, yd, zu, zd = up(c, 0), down(c, 0), up(c, 1), down(c, 1)
            total = ((n + s) + (yu + yd)) + (zu + zd)
            conv = w0 * (n - s) + w1 * (yu - yd) + w2 * (zu - zd)
            flux[d, p] = (7.0 * c - total + conv) * m

    loop(H - HW, H + nx + HW, momentum, 1)

    def product(p):
        f1, f2 = flux[1, p], flux[2, p]
        s = (flux[0, p + 1] - flux[0, p - 1]) + (up(f1, 0) - down(f1, 0)) + (up(f2, 1) - down(f2, 1))
        pr[p] = s * ((-0.5 * sx(p)) * m2[...])

    loop(H - 2, H + nx + 2, product)

    vb[H - 2] = jnp.zeros((ry, rz), jnp.float32)
    vb[H + nx + 1] = jnp.zeros((ry, rz), jnp.float32)
    pre(pr, vb, H - 1, H + nx + 1)

    fs[0] = vb[H + 1, H : H + ny, 0:nz]
    fs[1] = vb[H + nx - 2, H : H + ny, 0:nz]
    for i in range(nx):
        fs[2, i : i + 1] = vb[H + i, H + 1 : H + 2, 0:nz]
        fs[3, i : i + 1] = vb[H + i, H + ny - 2 : H + ny - 1, 0:nz]
    lo, hi = jnp.zeros((ny, nz), jnp.float32), jnp.zeros((ny, nz), jnp.float32)
    for i in range(nx):
        plane = vb[H + i, H : H + ny, 0:nz]
        lo = jnp.where(lane1 == i, pltpu.roll(plane, (nz + i - 1) % nz, 1), lo)
        hi = jnp.where(lane1 == i, pltpu.roll(plane, (i + 2) % nz, 1), hi)
    fs[4] = lo
    fs[5] = hi
    faces = [(-1, 0, 0), (1, 0, 0), (0, -1, 0), (0, 1, 0), (0, 0, -1), (0, 0, 1)]
    faces = [(k, d) for k, d in enumerate(faces) if d in offsets]

    def fcopy(k, d):
        return pltpu.make_async_remote_copy(
            src_ref=fs.at[k], dst_ref=fr.at[k], send_sem=fsend.at[k], recv_sem=frecv.at[k],
            device_id=(mx + d[0], my + d[1], mz + d[2]), device_id_type=MESH)

    coarse_source(1, pr, vb)
    for k, d in faces:
        pl.when(exists(*d))(lambda k=k, d=d: fcopy(k, d).start())
    coarse_gather(1)
    coarse(1)
    for k, d in faces:
        back = opposite(d)

        @pl.when(exists(*back))
        def _(k=k, d=d):
            fcopy(k, d).wait_recv()
            if k == 0:
                vb[H + nx + 1, H : H + ny, 0:nz] = fr[0]
            if k == 1:
                vb[H - 2, H : H + ny, 0:nz] = fr[1]
            if k == 2:
                for i in range(nx):
                    vb[H + i, H + ny + 1 : H + ny + 2, 0:nz] = fr[2, i : i + 1]
            if k == 3:
                for i in range(nx):
                    vb[H + i, H - 2 : H - 1, 0:nz] = fr[3, i : i + 1]
            if k == 4:
                for i in range(nx):
                    old = vb[H + i, H : H + ny, nz : 2 * nz]
                    new = pltpu.roll(fr[4], (nz + 1 - i) % nz, 1)
                    vb[H + i, H : H + ny, nz : 2 * nz] = jnp.where(lane1 == 1, new, old)
            if k == 5:
                for i in range(nx):
                    old = vb[H + i, H : H + ny, nz : 2 * nz]
                    new = pltpu.roll(fr[5], (nz - 2 - i) % nz, 1)
                    vb[H + i, H : H + ny, nz : 2 * nz] = jnp.where(lane1 == nz - 2, new, old)

    correct(vb, H - 2, H + nx + 2)
    post(pr, vb, va, H - 1, H + nx + 1)

    def finish(p):
        c = va[p]
        out = KEEP * c + CB0 * pr[p] + CS * six(va, p, c)
        o_ref[p - H] = out[H : H + ny, 0:nz]

    loop(H, H + nx, finish)

    for d in offsets:
        @pl.when(exists(*d))
        def _(d=d):
            pcopy(d).wait_send()
            wcopy(d).wait_send()
    peers(lambda t, ax, ay, dz: gcopy(0, t, ax, ay, dz, me).wait_send())
    peers(lambda t, ax, ay, dz: gcopy(1, t, ax, ay, dz, me).wait_send())
    for k, d in faces:
        pl.when(exists(*d))(lambda k=k, d=d: fcopy(k, d).wait_send())


def body(counts, pressure, wind):
    gx, gy, gz = counts
    nx, ny, nz = pressure.shape
    cx, cy = nx // 2, ny // 2
    rx, ry, rz = nx + 2 * H, ny + 2 * H, 2 * nz
    group = gx * gy
    x1, tr, hy = gx * cx, gy * cy + 8, gy * cy // 2
    V = lambda *shape: pltpu.VMEM(shape, jnp.float32)
    D = lambda *shape: pltpu.SemaphoreType.DMA(shape)
    scratch = [
        V(rx, ry, rz), V(rx, ry, rz), V(rx, ry, rz),
        V(3, rx, ry, rz), V(3, rx, ry, rz), V(3, nx + 2 * HW, ry, rz),
        V(ry, rz), V(2, 9, ny, nz), V(2, 9, ny, nz), V(2, ny, nz), V(2, ny, nz),
        V(cx, ny, nz), V(cx * cy, nz),
        V(x1 + 2, tr, nz), V(x1 + 2, tr, nz), V(x1 + 2, tr, nz),
        V(x1 // 2 + 2, hy, nz), V(2, x1 // 2 + 2, hy, nz), V(x1 + 2, tr, nz),
        V(rx // 2, 2, ry, nz), V(rx // 2 * (ry // 2), nz), V(tr, nz),
        V(2, cx // 2, cy, nz), V(2, 2, cy, nz),
        V(2, group, cx // 2, cy, nz), V(2, group, 2, cy, nz),
        V(6, ny, nz), V(6, ny, nz),
        D(27), D(27), D(27), D(27), D(2, group, 3), D(2, group, 3), D(6), D(6),
    ]
    return pl.pallas_call(
        functools.partial(kernel, counts, (nx, ny, nz)),
        out_shape=jax.ShapeDtypeStruct(pressure.shape, jnp.float32),
        in_specs=[pl.BlockSpec(memory_space=pltpu.VMEM)] * 2,
        out_specs=pl.BlockSpec(memory_space=pltpu.VMEM),
        scratch_shapes=scratch,
        compiler_params=pltpu.CompilerParams(collective_id=0, has_side_effects=True),
    )(pressure, wind)


def solution(mesh):
    counts = tuple(mesh.shape[name] for name in ("gx", "gy", "gz"))
    in_specs = (P("gx", "gy", "gz"), P(None, "gx", "gy", "gz"))
    return jax.shard_map(
        functools.partial(body, counts), mesh=mesh, in_specs=in_specs,
        out_specs=P("gx", "gy", "gz"), check_vma=False)
```

```python
import functools

import jax
import jax.numpy as jnp
from jax import lax
from jax.experimental import pallas as pl
from jax.experimental.pallas import tpu as pltpu
from jax.sharding import PartitionSpec as P

MESH = pl.DeviceIdType.MESH
OMEGA = 0.8
KEEP = 1.0 - OMEGA
CS = OMEGA / 6.0
H = 8
HW = 3
ZS = 8
L1S = 16
UNROLL = 6
NEAR = 2


def loop(low, high, step, unroll=UNROLL):
    def run(p, carry):
        step(p)
        return carry

    lax.fori_loop(low, high, run, 0, unroll=min(unroll, high - low))


def kernel(
    counts, local,
    p_ref, w_ref, o_ref,
    pr, va, vb, vel, flux, wr, m2, bz, wzr, pk, wpk,
    s16, cat, b1, v1, r1, b2, u2, e1, tmp, ex, tall,
    m1s, m2s, m1r, m2r, fs, fr,
    lsem, psend, precv, wsend, wrecv, gsend, grecv, fsend, frecv,
):
    gx, gy, gz = counts
    nx, ny, nz = local
    cx, cy, cz = nx // 2, ny // 2, nz // 2
    mx, my, mz = lax.axis_index("gx"), lax.axis_index("gy"), lax.axis_index("gz")
    me = mx * gy + my
    group = gx * gy

    def exists(dx, dy, dz):
        ok = None
        for d, m, g in ((dx, mx, gx), (dy, my, gy), (dz, mz, gz)):
            if d:
                here = (m + d >= 0) & (m + d < g)
                ok = here if ok is None else ok & here
        return ok

    own_p = pltpu.make_async_copy(
        p_ref, pr.at[pl.ds(H, nx), pl.ds(H, ny), pl.ds(0, nz)], lsem.at[0])
    own_w = pltpu.make_async_copy(
        w_ref, wr.at[:, pl.ds(HW, nx), pl.ds(H, ny), pl.ds(0, nz)], lsem.at[1])
    own_p.start()
    own_w.start()

    barrier = pltpu.get_barrier_semaphore()

    def peers(act):
        def at(t):
            ax, ay = t // gy, t % gy
            for dz in (-1, 0, 1):
                ok = (mz + dz >= 0) & (mz + dz < gz)
                if dz == 0:
                    ok = t != me

                @pl.when(ok)
                def _():
                    act(t, ax, ay, dz)

        loop(0, group, at, 1)

    peers(lambda t, ax, ay, dz: pl.semaphore_signal(
        barrier, inc=1, device_id=(ax, ay, mz + dz), device_id_type=MESH))

    row = lax.broadcasted_iota(jnp.int32, (ny + 2 * H, 2 * nz), 0) - H
    lane = lax.broadcasted_iota(jnp.int32, (ny + 2 * H, 2 * nz), 1)
    zpos = jnp.where(lane < nz + nz // 2, lane, lane - 2 * nz)
    inside = (
        (row + my * ny >= 0) & (row + my * ny < gy * ny)
        & (zpos + mz * nz >= 0) & (zpos + mz * nz < gz * nz)
    )
    m2[...] = inside.astype(jnp.float32)

    def sx(p):
        x = mx * nx + p - H
        return jnp.where((x >= 0) & (x < gx * nx), 1.0, 0.0).astype(jnp.float32)

    lane1 = lax.broadcasted_iota(jnp.int32, (ny, nz), 1)

    def pack(planes, width):
        lo, hi = jnp.zeros((ny, nz), jnp.float32), jnp.zeros((ny, nz), jnp.float32)
        for i, plane in enumerate(planes):
            at = width * i
            a = plane if at == 0 else pltpu.roll(plane, at, 1)
            b = pltpu.roll(plane, (at + width) % nz, 1)
            sel = (lane1 >= at) & (lane1 < at + width)
            lo = jnp.where(sel, a, lo)
            hi = jnp.where(sel, b, hi)
        return lo, hi

    own_p.wait()
    pk[0], pk[1] = pack([pr[H + i, H : H + ny, 0:nz] for i in range(nx)], ZS)

    n_peers = 3 * group - 1
    n_peers = n_peers - jnp.where(mz == 0, group, 0) - jnp.where(mz == gz - 1, group, 0)
    pl.semaphore_wait(barrier, n_peers)

    def span(d, n, h, skip=0):
        if d == 0:
            return 0, 0, n
        if d > 0:
            return n - skip - h, -skip - h, h
        return skip, n + skip, h

    offsets = [
        (dx, dy, dz) for dz in (0, -1, 1) for dx in (-1, 1, 0) for dy in (-1, 1, 0)
        if (dx, dy, dz) != (0, 0, 0)
        and (gx > 1 or dx == 0) and (gy > 1 or dy == 0) and (gz > 1 or dz == 0)
    ]

    def key(d):
        return (d[0] + 1) * 9 + (d[1] + 1) * 3 + d[2] + 1

    near = [(d, 0) for d in offsets if 0 in d]
    far = [(d, 1) for d in offsets if d[0] != 0 and (d[2] == 0 or d[1] != 0)]

    def edge(buf, got, d):
        ys, _, n = span(d[1], ny, H)
        side = 0 if d[2] < 0 else 1
        slot = (1 - d[0]) * 3 + 1 - d[1]
        return buf.at[side, pl.ds(ys, n)], got.at[side, slot, pl.ds(ys, n)]

    def pcopy(d, part):
        dx, dy, dz = d
        k = key(d) + 27 * part
        if dz == 0:
            xs, xd, n = span(dx, nx, H - NEAR if part else NEAR, NEAR if part else 0)
            ys, yd, m = span(dy, ny, H)
            src = pr.at[pl.ds(H + xs, n), pl.ds(H + ys, m), pl.ds(0, nz)]
            dst = pr.at[pl.ds(H + xd, n), pl.ds(H + yd, m), pl.ds(0, nz)]
        else:
            src, dst = edge(pk, bz, d)
        return pltpu.make_async_remote_copy(
            src_ref=src, dst_ref=dst, send_sem=psend.at[k], recv_sem=precv.at[k],
            device_id=(mx + dx, my + dy, mz + dz), device_id_type=MESH)

    def wcopy(d):
        dx, dy, dz = d
        k = key(d)
        if dz == 0:
            xs, xd, n = span(dx, nx, HW)
            ys, yd, m = span(dy, ny, H)
            src = wr.at[:, pl.ds(HW + xs, n), pl.ds(H + ys, m), pl.ds(0, nz)]
            dst = wr.at[:, pl.ds(HW + xd, n), pl.ds(H + yd, m), pl.ds(0, nz)]
        else:
            src, dst = edge(wpk, wzr, d)
        return pltpu.make_async_remote_copy(
            src_ref=src, dst_ref=dst, send_sem=wsend.at[k], recv_sem=wrecv.at[k],
            device_id=(mx + dx, my + dy, mz + dz), device_id_type=MESH)

    def opposite(d):
        return (-d[0], -d[1], -d[2])

    for d, part in near:
        pl.when(exists(*d))(lambda d=d, part=part: pcopy(d, part).start())

    for d, part in near:
        pl.when(exists(*opposite(d)))(lambda d=d, part=part: pcopy(d, part).wait_recv())

    def rows_of(buf, side, ix):
        parts = []
        for iy, (s, n) in enumerate(((ny - H, H), (0, ny), (0, H))):
            parts.append(buf[side, ix * 3 + iy, pl.ds(s, n), :])
        return jnp.concatenate(parts, axis=0)

    def unpack(buf_lo, buf_hi, at, width):
        lanes = lax.broadcasted_iota(jnp.int32, buf_lo.shape, 1)
        right = buf_lo if at == 0 else pltpu.roll(buf_lo, nz - at, 1)
        left = pltpu.roll(buf_hi, (2 * nz - width - at) % nz, 1)
        return jnp.where(lanes < width, right, jnp.where(lanes >= nz - width, left, 0.0))

    okmask = m2[...] > 0.5

    def plane_ok(p):
        x = mx * nx + p - H
        return okmask & ((x >= 0) & (x < gx * nx))

    right, left = rows_of(bz, 0, 1), rows_of(bz, 1, 1)
    for i in range(nx):
        p = H + i
        halo = unpack(right, left, ZS * i, ZS)
        pr[p, :, nz:] = jnp.where(okmask[:, nz:], halo, 0.0)
        for rows in (slice(0, H), slice(H + ny, 2 * H + ny)):
            pr[p, rows, 0:nz] = jnp.where(okmask[rows, :nz], pr[p, rows, 0:nz], 0.0)
    none = jnp.zeros((H, nz), jnp.float32)
    for ix, first, low in ((0, nx - NEAR, H - NEAR), (2, 0, H + nx)):
        right, left = bz[0, ix * 3 + 1], bz[1, ix * 3 + 1]
        for i in range(NEAR):
            p = low + i
            halo = unpack(right, left, ZS * (first + i), ZS)
            halo = jnp.concatenate([none, halo, none], axis=0)
            good = plane_ok(p)
            pr[p, :, 0:nz] = jnp.where(good[:, :nz], pr[p, :, 0:nz], 0.0)
            pr[p, :, nz:] = jnp.where(good[:, nz:], halo, 0.0)

    def far_planes():
        for ix, first, low in ((0, nx - H, 0), (2, 0, H + nx)):
            right, left = rows_of(bz, 0, ix), rows_of(bz, 1, ix)
            for i in range(H):
                p = low + i
                halo = unpack(right, left, ZS * (first + i), ZS)
                good = plane_ok(p)
                pr[p, :, 0:nz] = jnp.where(good[:, :nz], pr[p, :, 0:nz], 0.0)
                pr[p, :, nz:] = jnp.where(good[:, nz:], halo, 0.0)

    ry, rz = ny + 2 * H, 2 * nz

    def up(v, axis, k=1):
        return pltpu.roll(v, v.shape[axis] - k, axis)

    def down(v, axis, k=1):
        return pltpu.roll(v, k, axis)

    def six(ref, p, centre):
        return (
            (ref[p + 1] + ref[p - 1])
            + (up(centre, 0) + down(centre, 0))
            + (up(centre, 1) + down(centre, 1))
        )

    CB0 = OMEGA / 6.0

    def pre(src, dst, low, high):
        def at(p):
            c = src[p]
            dst[p] = (CB0 * (1.2 * c + CS * six(src, p, c))) * (sx(p) * m2[...])

        loop(low, high, at)

    li = lax.broadcasted_iota(jnp.int32, (nz, nz), 0)
    lj = lax.broadcasted_iota(jnp.int32, (nz, nz), 1)
    squeeze = jnp.where(li // 2 == lj % cz, 0.125, 0.0).astype(jnp.float32)
    ei = lax.broadcasted_iota(jnp.int32, (nz, 2 * nz), 0)
    ej = lax.broadcasted_iota(jnp.int32, (nz, 2 * nz), 1)
    spread = jnp.where(ej // 2 == ei, 1.0, 0.0).astype(jnp.float32)

    lane8 = lax.broadcasted_iota(jnp.int32, (cy, nz), 1)
    z1 = jnp.where(lane8 < nz - cz // 2, lane8, lane8 - nz)
    zin1 = (
        (z1 + mz * cz >= 0) & (z1 + mz * cz < gz * cz)
        & (z1 >= -L1S) & (z1 < cz + L1S)
    )
    tr = 8 + gy * cy
    row1 = lax.broadcasted_iota(jnp.int32, (tr, nz), 0)
    lan1 = lax.broadcasted_iota(jnp.int32, (tr, nz), 1)
    zl1 = jnp.where(lan1 < nz - cz // 2, lan1, lan1 - nz)
    mask1 = (
        (row1 >= 4) & (row1 < tr - 4)
        & (zl1 + mz * cz >= 0) & (zl1 + mz * cz < gz * cz)
    ).astype(jnp.float32)
    hy = gy * cy // 2
    row2 = lax.broadcasted_iota(jnp.int32, (hy, nz), 0)
    lan2 = lax.broadcasted_iota(jnp.int32, (hy, nz), 1)
    zl2 = jnp.where(lan2 < nz - cz // 2, lan2, lan2 - nz)
    mask2 = ((zl2 + mz * cz >= 0) & (zl2 + mz * cz < gz * cz)).astype(jnp.float32)
    not_first = (row2 > 0).astype(jnp.float32)
    not_last = (row2 < hy - 1).astype(jnp.float32)
    even2 = lan2 % 2 == 0

    X1 = gx * cx
    X2 = X1 // 2
    zero1 = jnp.zeros((tr, nz), jnp.float32)
    zero2 = jnp.zeros((hy, nz), jnp.float32)
    for ref in (b1, v1, r1, e1):
        ref[0] = zero1
        ref[X1 + 1] = zero1
    loop(1, X1 + 1, lambda p: b1.__setitem__(p, zero1))
    u2[0, 0] = zero2
    u2[0, X2 + 1] = zero2
    u2[1, 0] = zero2
    u2[1, X2 + 1] = zero2

    def gcopy(turn, t, ax, ay, dz, slot):
        side = dz + 1
        if dz == 0:
            src, dst = m1s.at[turn], m1r.at[turn, slot]
        else:
            src = m2s.at[turn, 0 if dz < 0 else 1]
            dst = m2r.at[turn, slot, 0 if dz < 0 else 1]
        return pltpu.make_async_remote_copy(
            src_ref=src, dst_ref=dst, send_sem=gsend.at[turn, t, side],
            recv_sem=grecv.at[turn, slot, side],
            device_id=(ax, ay, mz + dz), device_id_type=MESH)

    def coarse_source(turn, src, v):
        for i in range(cx):
            parts = []
            for q in (H + 2 * i, H + 2 * i + 1):
                c = v[q]
                r = src[q] - 6.0 * c + six(v, q, c)
                parts.append(r[H : H + ny, 0:nz])
            s16[i] = parts[0] + parts[1]
            cat[cy * i : cy * (i + 1)] = (
                s16[i, pl.ds(0, cy, stride=2), :] + s16[i, pl.ds(1, cy, stride=2), :]
            )
        c1 = lax.dot_general(
            cat[...], squeeze, (((1,), (0,)), ((), ())),
            precision=lax.Precision.HIGHEST, preferred_element_type=jnp.float32)
        planes = [c1[cy * i : cy * (i + 1)] for i in range(cx)]
        for i in range(cx // 2):
            m1s[turn, i] = jnp.where(lane8 < cz, planes[i], planes[i + cx // 2])
            m1r[turn, me, i] = jnp.where(lane8 < cz, planes[i], planes[i + cx // 2])
        lo = jnp.zeros((cy, nz), jnp.float32)
        hi = jnp.zeros((cy, nz), jnp.float32)
        for i in range(cx):
            sel = (lane8 >= L1S * i) & (lane8 < L1S * (i + 1))
            a = planes[i] if i == 0 else pltpu.roll(planes[i], L1S * i, 1)
            b = pltpu.roll(planes[i], (L1S * i + nz - cz + L1S) % nz, 1)
            lo = jnp.where(sel, a, lo)
            hi = jnp.where(sel, b, hi)
        m2s[turn, 0] = lo
        m2s[turn, 1] = hi
        peers(lambda t, ax, ay, dz: gcopy(turn, t, ax, ay, dz, me).start())

    def coarse_gather(turn):
        def at(t):
            ax, ay = t // gy, t % gy
            for dz in (-1, 0, 1):
                ok = (mz - dz >= 0) & (mz - dz < gz)
                if dz == 0:
                    ok = t != me

                @pl.when(ok)
                def _():
                    gcopy(turn, t, ax, ay, dz, t).wait_recv()

        loop(0, group, at, 1)
        for t in range(group):
            ax, ay = t // gy, t % gy
            for i in range(cx):
                body = m1r[turn, t, i % (cx // 2)]
                if i >= cx // 2:
                    body = pltpu.roll(body, cz, 1)
                right = pltpu.roll(m2r[turn, t, 0], (cz - L1S * i) % nz, 1)
                left = pltpu.roll(m2r[turn, t, 1], (2 * nz - L1S - L1S * i) % nz, 1)
                whole = jnp.where(lane8 < cz, body, jnp.where(lane8 < nz - L1S, right, left))
                b1[1 + ax * cx + i, 4 + cy * ay : 4 + cy * (ay + 1)] = jnp.where(zin1, whole, 0.0)

    def coarse(turn):
        cb1 = OMEGA / (6.0 * 0.25)
        cb2 = OMEGA / (6.0 * 0.0625)

        def at(p):
            c = b1[p]
            v1[p] = (cb1 * (1.2 * c + CS * six(b1, p, c))) * mask1

        loop(1, X1 + 1, at)

        def residual(p):
            c = v1[p]
            return b1[p] - 0.25 * (6.0 * c - six(v1, p, c))

        def down_to_2(j):
            tall[...] = residual(2 * j + 1) + residual(2 * j + 2)
            s = tall[pl.ds(4, hy, stride=2), :] + tall[pl.ds(5, hy, stride=2), :]
            s = s + jnp.where(even2, up(s, 1), down(s, 1))
            s = (0.125 * s) * mask2
            b2[j + 1] = s
            u2[0, j + 1] = cb2 * s

        loop(0, X2, down_to_2)
        for number in range(3):
            a, b = number % 2, (number + 1) % 2

            def sweep2(j, a=a, b=b):
                c = u2[a, j]
                s = (
                    (u2[a, j + 1] + u2[a, j - 1])
                    + (up(c, 0) * not_last + down(c, 0) * not_first)
                    + (up(c, 1, 2) + down(c, 1, 2))
                )
                u2[b, j] = (KEEP * c + cb2 * b2[j] + CS * s) * mask2

            loop(1, X2 + 1, sweep2)

        tall[...] = zero1

        def up_to_1(j):
            e = u2[1, j + 1]
            tall[pl.ds(4, hy, stride=2), :] = e
            tall[pl.ds(5, hy, stride=2), :] = e
            t = tall[...]
            v1[2 * j + 1] = v1[2 * j + 1] + t
            v1[2 * j + 2] = v1[2 * j + 2] + t

        loop(0, X2, up_to_1)
        for src, dst in ((v1, r1), (r1, e1)):
            def sweep1(p, src=src, dst=dst):
                c = src[p]
                dst[p] = (KEEP * c + cb1 * b1[p] + CS * six(src, p, c)) * mask1

            loop(1, X1 + 1, sweep1)

    half = ry // 2

    def correct(v, low, high):
        first = low // 2
        last = (high + 1) // 2
        n = last - first
        for k in range(n):
            x = mx * cx + first + k - H // 2
            x = jnp.clip(x, 0, X1 - 1) + 1
            ex[half * k : half * (k + 1)] = e1[x, pl.ds(pl.multiple_of(my * cy, 8), half), :]
        wide = lax.dot_general(
            ex[0 : half * n], spread, (((1,), (0,)), ((), ())),
            precision=lax.Precision.HIGHEST, preferred_element_type=jnp.float32)
        m = m2[...]
        for k in range(n):
            piece = wide[half * k : half * (k + 1)]
            for h in range(2):
                tmp[k, h, pl.ds(0, half, stride=2), :] = piece[:, h * nz : (h + 1) * nz]
                tmp[k, h, pl.ds(1, half, stride=2), :] = piece[:, h * nz : (h + 1) * nz]
            for q in (2 * (first + k), 2 * (first + k) + 1):
                if low <= q < high:
                    for h in range(2):
                        ls = slice(h * nz, (h + 1) * nz)
                        v[q, :, ls] = v[q, :, ls] + tmp[k, h] * (sx(q) * m[:, ls])

    def post(b, src, dst, low, high):
        def at(p):
            c = src[p]
            dst[p] = (KEEP * c + CB0 * b[p] + CS * six(src, p, c)) * (sx(p) * m2[...])

        loop(low, high, at)

    pre(pr, va, H - 1, H + nx + 1)
    coarse_source(0, pr, va)
    for d, part in far:
        pl.when(exists(*d))(lambda d=d, part=part: pcopy(d, part).start())
    own_w.wait()
    wpk[0], wpk[1] = pack(
        [wr[e, HW + i, H : H + ny, 0:nz] for e in range(3) for i in range(nx)], HW)
    for d in offsets:
        pl.when(exists(*d))(lambda d=d: wcopy(d).start())
    coarse_gather(0)
    coarse(0)
    for d, part in far:
        pl.when(exists(*opposite(d)))(lambda d=d, part=part: pcopy(d, part).wait_recv())
    far_planes()
    pre(pr, va, 1, H + 1)
    pre(pr, va, H + nx - 1, nx + 2 * H - 1)
    correct(va, 1, nx + 2 * H - 1)
    post(pr, va, vb, 2, nx + 2 * H - 2)
    post(pr, vb, va, 3, nx + 2 * H - 3)

    def velocity(p):
        c = va[p]
        m = (0.5 * sx(p)) * m2[...]
        vel[0, p] = (va[p + 1] - va[p - 1]) * m
        vel[1, p] = (up(c, 0) - down(c, 0)) * m
        vel[2, p] = (up(c, 1) - down(c, 1)) * m

    loop(4, nx + 2 * H - 4, velocity)

    for d in offsets:
        pl.when(exists(*opposite(d)))(lambda d=d: wcopy(d).wait_recv())
    for ix, (first, low, n) in enumerate(((nx - HW, 0, HW), (0, HW, nx), (0, HW + nx, HW))):
        right, left = rows_of(wzr, 0, ix), rows_of(wzr, 1, ix)
        for e in range(3):
            for i in range(n):
                wr[e, low + i, :, nz:] = unpack(right, left, HW * (e * nx + first + i), HW)

    def momentum(p):
        m = sx(p) * m2[...] > 0.5
        q = p - (H - HW)
        w0, w1, w2 = 0.5 * wr[0, q], 0.5 * wr[1, q], 0.5 * wr[2, q]
        for d in range(3):
            c, n, s = vel[d, p], vel[d, p + 1], vel[d, p - 1]
            yu, yd, zu, zd = up(c, 0), down(c, 0), up(c, 1), down(c, 1)
            total = ((n + s) + (yu + yd)) + (zu + zd)
            conv = w0 * (n - s) + w1 * (yu - yd) + w2 * (zu - zd)
            flux[d, p] = jnp.where(m, 7.0 * c - total + conv, 0.0)

    loop(H - HW, H + nx + HW, momentum, 1)
    for d, part in near + far:
        pl.when(exists(*d))(lambda d=d, part=part: pcopy(d, part).wait_send())

    def product(p):
        f1, f2 = flux[1, p], flux[2, p]
        s = (flux[0, p + 1] - flux[0, p - 1]) + (up(f1, 0) - down(f1, 0)) + (up(f2, 1) - down(f2, 1))
        pr[p] = s * ((-0.5 * sx(p)) * m2[...])

    loop(H - 2, H + nx + 2, product)

    vb[H - 2] = jnp.zeros((ry, rz), jnp.float32)
    vb[H + nx + 1] = jnp.zeros((ry, rz), jnp.float32)
    pre(pr, vb, H - 1, H + nx + 1)

    fs[0] = vb[H + 1, H : H + ny, 0:nz]
    fs[1] = vb[H + nx - 2, H : H + ny, 0:nz]
    for i in range(nx):
        fs[2, i : i + 1] = vb[H + i, H + 1 : H + 2, 0:nz]
        fs[3, i : i + 1] = vb[H + i, H + ny - 2 : H + ny - 1, 0:nz]
    lo, hi = jnp.zeros((ny, nz), jnp.float32), jnp.zeros((ny, nz), jnp.float32)
    for i in range(nx):
        plane = vb[H + i, H : H + ny, 0:nz]
        lo = jnp.where(lane1 == i, pltpu.roll(plane, (nz + i - 1) % nz, 1), lo)
        hi = jnp.where(lane1 == i, pltpu.roll(plane, (i + 2) % nz, 1), hi)
    fs[4] = lo
    fs[5] = hi
    faces = [(-1, 0, 0), (1, 0, 0), (0, -1, 0), (0, 1, 0), (0, 0, -1), (0, 0, 1)]
    faces = [(k, d) for k, d in enumerate(faces) if d in offsets]

    def fcopy(k, d):
        return pltpu.make_async_remote_copy(
            src_ref=fs.at[k], dst_ref=fr.at[k], send_sem=fsend.at[k], recv_sem=frecv.at[k],
            device_id=(mx + d[0], my + d[1], mz + d[2]), device_id_type=MESH)

    coarse_source(1, pr, vb)
    for k, d in faces:
        pl.when(exists(*d))(lambda k=k, d=d: fcopy(k, d).start())
    coarse_gather(1)
    coarse(1)
    for k, d in faces:
        back = opposite(d)

        @pl.when(exists(*back))
        def _(k=k, d=d):
            fcopy(k, d).wait_recv()
            if k == 0:
                vb[H + nx + 1, H : H + ny, 0:nz] = fr[0]
            if k == 1:
                vb[H - 2, H : H + ny, 0:nz] = fr[1]
            if k == 2:
                for i in range(nx):
                    vb[H + i, H + ny + 1 : H + ny + 2, 0:nz] = fr[2, i : i + 1]
            if k == 3:
                for i in range(nx):
                    vb[H + i, H - 2 : H - 1, 0:nz] = fr[3, i : i + 1]
            if k == 4:
                for i in range(nx):
                    old = vb[H + i, H : H + ny, nz : 2 * nz]
                    new = pltpu.roll(fr[4], (nz + 1 - i) % nz, 1)
                    vb[H + i, H : H + ny, nz : 2 * nz] = jnp.where(lane1 == 1, new, old)
            if k == 5:
                for i in range(nx):
                    old = vb[H + i, H : H + ny, nz : 2 * nz]
                    new = pltpu.roll(fr[5], (nz - 2 - i) % nz, 1)
                    vb[H + i, H : H + ny, nz : 2 * nz] = jnp.where(lane1 == nz - 2, new, old)

    correct(vb, H - 2, H + nx + 2)
    post(pr, vb, va, H - 1, H + nx + 1)

    def finish(p):
        c = va[p]
        out = KEEP * c + CB0 * pr[p] + CS * six(va, p, c)
        o_ref[p - H] = out[H : H + ny, 0:nz]

    loop(H, H + nx, finish)

    for d in offsets:
        @pl.when(exists(*d))
        def _(d=d):
            wcopy(d).wait_send()
    peers(lambda t, ax, ay, dz: gcopy(0, t, ax, ay, dz, me).wait_send())
    peers(lambda t, ax, ay, dz: gcopy(1, t, ax, ay, dz, me).wait_send())
    for k, d in faces:
        pl.when(exists(*d))(lambda k=k, d=d: fcopy(k, d).wait_send())


def body(counts, pressure, wind):
    gx, gy, gz = counts
    nx, ny, nz = pressure.shape
    cx, cy = nx // 2, ny // 2
    rx, ry, rz = nx + 2 * H, ny + 2 * H, 2 * nz
    group = gx * gy
    x1, tr, hy = gx * cx, gy * cy + 8, gy * cy // 2
    V = lambda *shape: pltpu.VMEM(shape, jnp.float32)
    D = lambda *shape: pltpu.SemaphoreType.DMA(shape)
    scratch = [
        V(rx, ry, rz), V(rx, ry, rz), V(rx, ry, rz),
        V(3, rx, ry, rz), V(3, rx, ry, rz), V(3, nx + 2 * HW, ry, rz),
        V(ry, rz), V(2, 9, ny, nz), V(2, 9, ny, nz), V(2, ny, nz), V(2, ny, nz),
        V(cx, ny, nz), V(cx * cy, nz),
        V(x1 + 2, tr, nz), V(x1 + 2, tr, nz), V(x1 + 2, tr, nz),
        V(x1 // 2 + 2, hy, nz), V(2, x1 // 2 + 2, hy, nz), V(x1 + 2, tr, nz),
        V(rx // 2, 2, ry, nz), V(rx // 2 * (ry // 2), nz), V(tr, nz),
        V(2, cx // 2, cy, nz), V(2, 2, cy, nz),
        V(2, group, cx // 2, cy, nz), V(2, group, 2, cy, nz),
        V(6, ny, nz), V(6, ny, nz),
        D(2), D(54), D(54), D(27), D(27), D(2, group, 3), D(2, group, 3), D(6), D(6),
    ]
    return pl.pallas_call(
        functools.partial(kernel, counts, (nx, ny, nz)),
        out_shape=jax.ShapeDtypeStruct(pressure.shape, jnp.float32),
        in_specs=[pl.BlockSpec(memory_space=pl.ANY)] * 2,
        out_specs=pl.BlockSpec(memory_space=pltpu.VMEM),
        scratch_shapes=scratch,
        compiler_params=pltpu.CompilerParams(collective_id=0, has_side_effects=True),
    )(pressure, wind)


def solution(mesh):
    counts = tuple(mesh.shape[name] for name in ("gx", "gy", "gz"))
    in_specs = (P("gx", "gy", "gz"), P(None, "gx", "gy", "gz"))
    return jax.shard_map(
        functools.partial(body, counts), mesh=mesh, in_specs=in_specs,
        out_specs=P("gx", "gy", "gz"), check_vma=False)
```

```python
import functools

import jax
import jax.numpy as jnp
from jax import lax
from jax.experimental import pallas as pl
from jax.experimental.pallas import tpu as pltpu
from jax.sharding import PartitionSpec as P

MESH = pl.DeviceIdType.MESH
OMEGA = 0.8
KEEP = 1.0 - OMEGA
CS = OMEGA / 6.0
H = 8
HW = 3
ZS = 8
DEEP = 14
L1S = 16
UNROLL = 12
NEAR = 2


def loop(low, high, step, unroll=UNROLL):
    def run(p, carry):
        step(p)
        return carry

    lax.fori_loop(low, high, run, 0, unroll=min(unroll, high - low))


def kernel(
    counts, local,
    p_ref, w_ref, o_ref,
    pr, va, vb, vel, flux, wr, m2, bz, wzr, pk, wpk,
    s16, cat, b1, v1, r1, b2, u2, e1, tmp, ex, tall,
    m1s, m2s, m1r, m2r, fs, fr,
    lsem, psend, precv, wsend, wrecv, gsend, grecv, fsend, frecv,
):
    gx, gy, gz = counts
    nx, ny, nz = local
    cx, cy, cz = nx // 2, ny // 2, nz // 2
    mx, my, mz = lax.axis_index("gx"), lax.axis_index("gy"), lax.axis_index("gz")
    me = mx * gy + my
    group = gx * gy

    def exists(dx, dy, dz):
        ok = None
        for d, m, g in ((dx, mx, gx), (dy, my, gy), (dz, mz, gz)):
            if d:
                here = (m + d >= 0) & (m + d < g)
                ok = here if ok is None else ok & here
        return ok

    own_p = pltpu.make_async_copy(
        p_ref, pr.at[pl.ds(H, nx), pl.ds(H, ny), pl.ds(0, nz)], lsem.at[0])
    own_w = pltpu.make_async_copy(
        w_ref, wr.at[:, pl.ds(HW, nx), pl.ds(H, ny), pl.ds(0, nz)], lsem.at[1])
    own_p.start()
    own_w.start()

    barrier = pltpu.get_barrier_semaphore()

    def reached(ax, ay):
        return (abs(ax - mx) <= -(-DEEP // cx)) & (abs(ay - my) <= -(-DEEP // cy))

    def peers(act):
        def at(t):
            ax, ay = t // gy, t % gy
            for dz in (-1, 0, 1):
                ok = (mz + dz >= 0) & (mz + dz < gz)
                if dz == 0:
                    ok = t != me

                @pl.when(ok & reached(ax, ay))
                def _():
                    act(t, ax, ay, dz)

        loop(0, group, at, 1)

    peers(lambda t, ax, ay, dz: pl.semaphore_signal(
        barrier, inc=1, device_id=(ax, ay, mz + dz), device_id_type=MESH))

    row = lax.broadcasted_iota(jnp.int32, (ny + 2 * H, 2 * nz), 0) - H
    lane = lax.broadcasted_iota(jnp.int32, (ny + 2 * H, 2 * nz), 1)
    zpos = jnp.where(lane < nz + nz // 2, lane, lane - 2 * nz)
    inside = (
        (row + my * ny >= 0) & (row + my * ny < gy * ny)
        & (zpos + mz * nz >= 0) & (zpos + mz * nz < gz * nz)
    )
    m2[...] = inside.astype(jnp.float32)

    def sx(p):
        x = mx * nx + p - H
        return jnp.where((x >= 0) & (x < gx * nx), 1.0, 0.0).astype(jnp.float32)

    lane1 = lax.broadcasted_iota(jnp.int32, (ny, nz), 1)

    def pack(planes, width):
        lo, hi = jnp.zeros((ny, nz), jnp.float32), jnp.zeros((ny, nz), jnp.float32)
        for i, plane in enumerate(planes):
            at = width * i
            a = plane if at == 0 else pltpu.roll(plane, at, 1)
            b = pltpu.roll(plane, (at + width) % nz, 1)
            sel = (lane1 >= at) & (lane1 < at + width)
            lo = jnp.where(sel, a, lo)
            hi = jnp.where(sel, b, hi)
        return lo, hi

    own_p.wait()
    pk[0], pk[1] = pack([pr[H + i, H : H + ny, 0:nz] for i in range(nx)], ZS)

    rx, ry = -(-DEEP // cx), -(-DEEP // cy)
    wide = jnp.minimum(mx + rx, gx - 1) - jnp.maximum(mx - rx, 0) + 1
    tall_ = jnp.minimum(my + ry, gy - 1) - jnp.maximum(my - ry, 0) + 1
    deep = jnp.minimum(mz + 1, gz - 1) - jnp.maximum(mz - 1, 0) + 1
    n_peers = wide * tall_ * deep - 1
    pl.semaphore_wait(barrier, n_peers)

    def span(d, n, h, skip=0):
        if d == 0:
            return 0, 0, n
        if d > 0:
            return n - skip - h, -skip - h, h
        return skip, n + skip, h

    offsets = [
        (dx, dy, dz) for dz in (0, -1, 1) for dx in (-1, 1, 0) for dy in (-1, 1, 0)
        if (dx, dy, dz) != (0, 0, 0)
        and (gx > 1 or dx == 0) and (gy > 1 or dy == 0) and (gz > 1 or dz == 0)
    ]

    def key(d):
        return (d[0] + 1) * 9 + (d[1] + 1) * 3 + d[2] + 1

    near = [(d, 0) for d in offsets if 0 in d]
    far = [(d, 1) for d in offsets if d[0] != 0 and (d[2] == 0 or d[1] != 0)]

    def edge(buf, got, d):
        ys, _, n = span(d[1], ny, H)
        side = 0 if d[2] < 0 else 1
        slot = (1 - d[0]) * 3 + 1 - d[1]
        return buf.at[side, pl.ds(ys, n)], got.at[side, slot, pl.ds(ys, n)]

    def pcopy(d, part):
        dx, dy, dz = d
        k = key(d) + 27 * part
        if dz == 0:
            xs, xd, n = span(dx, nx, H - NEAR if part else NEAR, NEAR if part else 0)
            ys, yd, m = span(dy, ny, H)
            src = pr.at[pl.ds(H + xs, n), pl.ds(H + ys, m), pl.ds(0, nz)]
            dst = pr.at[pl.ds(H + xd, n), pl.ds(H + yd, m), pl.ds(0, nz)]
        else:
            src, dst = edge(pk, bz, d)
        return pltpu.make_async_remote_copy(
            src_ref=src, dst_ref=dst, send_sem=psend.at[k], recv_sem=precv.at[k],
            device_id=(mx + dx, my + dy, mz + dz), device_id_type=MESH)

    def wcopy(d):
        dx, dy, dz = d
        k = key(d)
        if dz == 0:
            xs, xd, n = span(dx, nx, HW)
            ys, yd, m = span(dy, ny, H)
            src = wr.at[:, pl.ds(HW + xs, n), pl.ds(H + ys, m), pl.ds(0, nz)]
            dst = wr.at[:, pl.ds(HW + xd, n), pl.ds(H + yd, m), pl.ds(0, nz)]
        else:
            src, dst = edge(wpk, wzr, d)
        return pltpu.make_async_remote_copy(
            src_ref=src, dst_ref=dst, send_sem=wsend.at[k], recv_sem=wrecv.at[k],
            device_id=(mx + dx, my + dy, mz + dz), device_id_type=MESH)

    def opposite(d):
        return (-d[0], -d[1], -d[2])

    for d, part in near:
        pl.when(exists(*d))(lambda d=d, part=part: pcopy(d, part).start())

    for d, part in near:
        pl.when(exists(*opposite(d)))(lambda d=d, part=part: pcopy(d, part).wait_recv())

    def rows_of(buf, side, ix):
        parts = []
        for iy, (s, n) in enumerate(((ny - H, H), (0, ny), (0, H))):
            parts.append(buf[side, ix * 3 + iy, pl.ds(s, n), :])
        return jnp.concatenate(parts, axis=0)

    def unpack(buf_lo, buf_hi, at, width):
        lanes = lax.broadcasted_iota(jnp.int32, buf_lo.shape, 1)
        right = buf_lo if at == 0 else pltpu.roll(buf_lo, nz - at, 1)
        left = pltpu.roll(buf_hi, (2 * nz - width - at) % nz, 1)
        return jnp.where(lanes < width, right, jnp.where(lanes >= nz - width, left, 0.0))

    okmask = m2[...] > 0.5

    def plane_ok(p):
        x = mx * nx + p - H
        return okmask & ((x >= 0) & (x < gx * nx))

    right, left = rows_of(bz, 0, 1), rows_of(bz, 1, 1)
    for i in range(nx):
        p = H + i
        halo = unpack(right, left, ZS * i, ZS)
        pr[p, :, nz:] = jnp.where(okmask[:, nz:], halo, 0.0)
        for rows in (slice(0, H), slice(H + ny, 2 * H + ny)):
            pr[p, rows, 0:nz] = jnp.where(okmask[rows, :nz], pr[p, rows, 0:nz], 0.0)
    none = jnp.zeros((H, nz), jnp.float32)
    for ix, first, low in ((0, nx - NEAR, H - NEAR), (2, 0, H + nx)):
        right, left = bz[0, ix * 3 + 1], bz[1, ix * 3 + 1]
        for i in range(NEAR):
            p = low + i
            halo = unpack(right, left, ZS * (first + i), ZS)
            halo = jnp.concatenate([none, halo, none], axis=0)
            good = plane_ok(p)
            pr[p, :, 0:nz] = jnp.where(good[:, :nz], pr[p, :, 0:nz], 0.0)
            pr[p, :, nz:] = jnp.where(good[:, nz:], halo, 0.0)

    def far_planes():
        for ix, first, low in ((0, nx - H, 0), (2, 0, H + nx)):
            right, left = rows_of(bz, 0, ix), rows_of(bz, 1, ix)
            for i in range(H):
                p = low + i
                halo = unpack(right, left, ZS * (first + i), ZS)
                good = plane_ok(p)
                pr[p, :, 0:nz] = jnp.where(good[:, :nz], pr[p, :, 0:nz], 0.0)
                pr[p, :, nz:] = jnp.where(good[:, nz:], halo, 0.0)

    ry, rz = ny + 2 * H, 2 * nz

    def up(v, axis, k=1):
        return pltpu.roll(v, v.shape[axis] - k, axis)

    def down(v, axis, k=1):
        return pltpu.roll(v, k, axis)

    def six(ref, p, centre):
        return (
            (ref[p + 1] + ref[p - 1])
            + (up(centre, 0) + down(centre, 0))
            + (up(centre, 1) + down(centre, 1))
        )

    CB0 = OMEGA / 6.0

    def pre(src, dst, low, high):
        def at(p):
            c = src[p]
            dst[p] = (CB0 * (1.2 * c + CS * six(src, p, c))) * (sx(p) * m2[...])

        loop(low, high, at)

    li = lax.broadcasted_iota(jnp.int32, (nz, nz), 0)
    lj = lax.broadcasted_iota(jnp.int32, (nz, nz), 1)
    squeeze = jnp.where(li // 2 == lj % cz, 0.125, 0.0).astype(jnp.float32)
    ei = lax.broadcasted_iota(jnp.int32, (nz, 2 * nz), 0)
    ej = lax.broadcasted_iota(jnp.int32, (nz, 2 * nz), 1)
    spread = jnp.where(ej // 2 == ei, 1.0, 0.0).astype(jnp.float32)

    lane8 = lax.broadcasted_iota(jnp.int32, (cy, nz), 1)
    z1 = jnp.where(lane8 < nz - cz // 2, lane8, lane8 - nz)
    zin1 = (
        (z1 + mz * cz >= 0) & (z1 + mz * cz < gz * cz)
        & (z1 >= -L1S) & (z1 < cz + L1S)
    )
    tr = 8 + gy * cy
    row1 = lax.broadcasted_iota(jnp.int32, (tr, nz), 0)
    lan1 = lax.broadcasted_iota(jnp.int32, (tr, nz), 1)
    zl1 = jnp.where(lan1 < nz - cz // 2, lan1, lan1 - nz)
    mask1 = (
        (row1 >= 4) & (row1 < tr - 4)
        & (zl1 + mz * cz >= 0) & (zl1 + mz * cz < gz * cz)
    ).astype(jnp.float32)
    hy = gy * cy // 2
    row2 = lax.broadcasted_iota(jnp.int32, (hy, nz), 0)
    lan2 = lax.broadcasted_iota(jnp.int32, (hy, nz), 1)
    zl2 = jnp.where(lan2 < nz - cz // 2, lan2, lan2 - nz)
    mask2 = ((zl2 + mz * cz >= 0) & (zl2 + mz * cz < gz * cz)).astype(jnp.float32)
    not_first = (row2 > 0).astype(jnp.float32)
    not_last = (row2 < hy - 1).astype(jnp.float32)
    even2 = lan2 % 2 == 0

    X1 = gx * cx
    X2 = X1 // 2
    zero1 = jnp.zeros((tr, nz), jnp.float32)
    zero2 = jnp.zeros((hy, nz), jnp.float32)
    for ref in (b1, v1, r1, e1):
        ref[0] = zero1
        ref[X1 + 1] = zero1
    loop(1, X1 + 1, lambda p: b1.__setitem__(p, zero1))
    u2[0, 0] = zero2
    u2[0, X2 + 1] = zero2
    u2[1, 0] = zero2
    u2[1, X2 + 1] = zero2

    def gcopy(turn, t, ax, ay, dz, slot):
        side = dz + 1
        if dz == 0:
            src, dst = m1s.at[turn], m1r.at[turn, slot]
        else:
            src = m2s.at[turn, 0 if dz < 0 else 1]
            dst = m2r.at[turn, slot, 0 if dz < 0 else 1]
        return pltpu.make_async_remote_copy(
            src_ref=src, dst_ref=dst, send_sem=gsend.at[turn, t, side],
            recv_sem=grecv.at[turn, slot, side],
            device_id=(ax, ay, mz + dz), device_id_type=MESH)

    def coarse_source(turn, src, v):
        for i in range(cx):
            parts = []
            for q in (H + 2 * i, H + 2 * i + 1):
                c = v[q]
                r = src[q] - 6.0 * c + six(v, q, c)
                parts.append(r[H : H + ny, 0:nz])
            s16[i] = parts[0] + parts[1]
            cat[cy * i : cy * (i + 1)] = (
                s16[i, pl.ds(0, cy, stride=2), :] + s16[i, pl.ds(1, cy, stride=2), :]
            )
        c1 = lax.dot_general(
            cat[...], squeeze, (((1,), (0,)), ((), ())),
            precision=lax.Precision.HIGHEST, preferred_element_type=jnp.float32)
        planes = [c1[cy * i : cy * (i + 1)] for i in range(cx)]
        for i in range(cx // 2):
            m1s[turn, i] = jnp.where(lane8 < cz, planes[i], planes[i + cx // 2])
            m1r[turn, me, i] = jnp.where(lane8 < cz, planes[i], planes[i + cx // 2])
        lo = jnp.zeros((cy, nz), jnp.float32)
        hi = jnp.zeros((cy, nz), jnp.float32)
        for i in range(cx):
            sel = (lane8 >= L1S * i) & (lane8 < L1S * (i + 1))
            a = planes[i] if i == 0 else pltpu.roll(planes[i], L1S * i, 1)
            b = pltpu.roll(planes[i], (L1S * i + nz - cz + L1S) % nz, 1)
            lo = jnp.where(sel, a, lo)
            hi = jnp.where(sel, b, hi)
        m2s[turn, 0] = lo
        m2s[turn, 1] = hi
        peers(lambda t, ax, ay, dz: gcopy(turn, t, ax, ay, dz, me).start())

    def coarse_gather(turn):
        def at(t):
            ax, ay = t // gy, t % gy
            for dz in (-1, 0, 1):
                ok = (mz - dz >= 0) & (mz - dz < gz)
                if dz == 0:
                    ok = t != me

                @pl.when(ok & reached(ax, ay))
                def _():
                    gcopy(turn, t, ax, ay, dz, t).wait_recv()

        loop(0, group, at, 1)
        for t in range(group):
            ax, ay = t // gy, t % gy
            for i in range(cx):
                body = m1r[turn, t, i % (cx // 2)]
                if i >= cx // 2:
                    body = pltpu.roll(body, cz, 1)
                right = pltpu.roll(m2r[turn, t, 0], (cz - L1S * i) % nz, 1)
                left = pltpu.roll(m2r[turn, t, 1], (2 * nz - L1S - L1S * i) % nz, 1)
                whole = jnp.where(lane8 < cz, body, jnp.where(lane8 < nz - L1S, right, left))
                b1[1 + ax * cx + i, 4 + cy * ay : 4 + cy * (ay + 1)] = jnp.where(zin1 & reached(ax, ay), whole, 0.0)

    def coarse(turn):
        cb1 = OMEGA / (6.0 * 0.25)
        cb2 = OMEGA / (6.0 * 0.0625)

        def at(p):
            c = b1[p]
            v1[p] = (cb1 * (1.2 * c + CS * six(b1, p, c))) * mask1

        loop(1, X1 + 1, at)

        def residual(p):
            c = v1[p]
            return b1[p] - 0.25 * (6.0 * c - six(v1, p, c))

        def down_to_2(j):
            tall[...] = residual(2 * j + 1) + residual(2 * j + 2)
            s = tall[pl.ds(4, hy, stride=2), :] + tall[pl.ds(5, hy, stride=2), :]
            s = s + jnp.where(even2, up(s, 1), down(s, 1))
            s = (0.125 * s) * mask2
            b2[j + 1] = s
            u2[0, j + 1] = cb2 * s

        loop(0, X2, down_to_2)
        for number in range(3):
            a, b = number % 2, (number + 1) % 2

            def sweep2(j, a=a, b=b):
                c = u2[a, j]
                s = (
                    (u2[a, j + 1] + u2[a, j - 1])
                    + (up(c, 0) * not_last + down(c, 0) * not_first)
                    + (up(c, 1, 2) + down(c, 1, 2))
                )
                u2[b, j] = (KEEP * c + cb2 * b2[j] + CS * s) * mask2

            loop(1, X2 + 1, sweep2)

        tall[...] = zero1

        def up_to_1(j):
            e = u2[1, j + 1]
            tall[pl.ds(4, hy, stride=2), :] = e
            tall[pl.ds(5, hy, stride=2), :] = e
            t = tall[...]
            v1[2 * j + 1] = v1[2 * j + 1] + t
            v1[2 * j + 2] = v1[2 * j + 2] + t

        loop(0, X2, up_to_1)
        for src, dst in ((v1, r1), (r1, e1)):
            def sweep1(p, src=src, dst=dst):
                c = src[p]
                dst[p] = (KEEP * c + cb1 * b1[p] + CS * six(src, p, c)) * mask1

            loop(1, X1 + 1, sweep1)

    half = ry // 2

    def correct(v, low, high):
        first = low // 2
        last = (high + 1) // 2
        n = last - first
        for k in range(n):
            x = mx * cx + first + k - H // 2
            x = jnp.clip(x, 0, X1 - 1) + 1
            ex[half * k : half * (k + 1)] = e1[x, pl.ds(pl.multiple_of(my * cy, 8), half), :]
        wide = lax.dot_general(
            ex[0 : half * n], spread, (((1,), (0,)), ((), ())),
            precision=lax.Precision.HIGHEST, preferred_element_type=jnp.float32)
        m = m2[...]
        for k in range(n):
            piece = wide[half * k : half * (k + 1)]
            for h in range(2):
                tmp[k, h, pl.ds(0, half, stride=2), :] = piece[:, h * nz : (h + 1) * nz]
                tmp[k, h, pl.ds(1, half, stride=2), :] = piece[:, h * nz : (h + 1) * nz]
            for q in (2 * (first + k), 2 * (first + k) + 1):
                if low <= q < high:
                    for h in range(2):
                        ls = slice(h * nz, (h + 1) * nz)
                        v[q, :, ls] = v[q, :, ls] + tmp[k, h] * (sx(q) * m[:, ls])

    def post(b, src, dst, low, high):
        def at(p):
            c = src[p]
            dst[p] = (KEEP * c + CB0 * b[p] + CS * six(src, p, c)) * (sx(p) * m2[...])

        loop(low, high, at)

    pre(pr, va, H - 1, H + nx + 1)
    coarse_source(0, pr, va)
    for d, part in far:
        pl.when(exists(*d))(lambda d=d, part=part: pcopy(d, part).start())
    own_w.wait()
    wpk[0], wpk[1] = pack(
        [wr[e, HW + i, H : H + ny, 0:nz] for e in range(3) for i in range(nx)], HW)
    for d in offsets:
        pl.when(exists(*d))(lambda d=d: wcopy(d).start())
    coarse_gather(0)
    coarse(0)
    for d, part in far:
        pl.when(exists(*opposite(d)))(lambda d=d, part=part: pcopy(d, part).wait_recv())
    far_planes()
    pre(pr, va, 1, H + 1)
    pre(pr, va, H + nx - 1, nx + 2 * H - 1)
    correct(va, 1, nx + 2 * H - 1)
    post(pr, va, vb, 2, nx + 2 * H - 2)
    post(pr, vb, va, 3, nx + 2 * H - 3)

    def velocity(p):
        c = va[p]
        m = (0.5 * sx(p)) * m2[...]
        vel[0, p] = (va[p + 1] - va[p - 1]) * m
        vel[1, p] = (up(c, 0) - down(c, 0)) * m
        vel[2, p] = (up(c, 1) - down(c, 1)) * m

    loop(4, nx + 2 * H - 4, velocity)

    for d in offsets:
        pl.when(exists(*opposite(d)))(lambda d=d: wcopy(d).wait_recv())
    for ix, (first, low, n) in enumerate(((nx - HW, 0, HW), (0, HW, nx), (0, HW + nx, HW))):
        right, left = rows_of(wzr, 0, ix), rows_of(wzr, 1, ix)
        for e in range(3):
            for i in range(n):
                wr[e, low + i, :, nz:] = unpack(right, left, HW * (e * nx + first + i), HW)

    def momentum(p):
        m = sx(p) * m2[...] > 0.5
        q = p - (H - HW)
        w0, w1, w2 = 0.5 * wr[0, q], 0.5 * wr[1, q], 0.5 * wr[2, q]
        for d in range(3):
            c, n, s = vel[d, p], vel[d, p + 1], vel[d, p - 1]
            yu, yd, zu, zd = up(c, 0), down(c, 0), up(c, 1), down(c, 1)
            total = ((n + s) + (yu + yd)) + (zu + zd)
            conv = w0 * (n - s) + w1 * (yu - yd) + w2 * (zu - zd)
            flux[d, p] = jnp.where(m, 7.0 * c - total + conv, 0.0)

    loop(H - HW, H + nx + HW, momentum, 3)
    for d, part in near + far:
        pl.when(exists(*d))(lambda d=d, part=part: pcopy(d, part).wait_send())

    def product(p):
        f1, f2 = flux[1, p], flux[2, p]
        s = (flux[0, p + 1] - flux[0, p - 1]) + (up(f1, 0) - down(f1, 0)) + (up(f2, 1) - down(f2, 1))
        pr[p] = s * ((-0.5 * sx(p)) * m2[...])

    loop(H - 2, H + nx + 2, product)

    vb[H - 2] = jnp.zeros((ry, rz), jnp.float32)
    vb[H + nx + 1] = jnp.zeros((ry, rz), jnp.float32)
    pre(pr, vb, H - 1, H + nx + 1)

    fs[0] = vb[H + 1, H : H + ny, 0:nz]
    fs[1] = vb[H + nx - 2, H : H + ny, 0:nz]
    for i in range(nx):
        fs[2, i : i + 1] = vb[H + i, H + 1 : H + 2, 0:nz]
        fs[3, i : i + 1] = vb[H + i, H + ny - 2 : H + ny - 1, 0:nz]
    lo, hi = jnp.zeros((ny, nz), jnp.float32), jnp.zeros((ny, nz), jnp.float32)
    for i in range(nx):
        plane = vb[H + i, H : H + ny, 0:nz]
        lo = jnp.where(lane1 == i, pltpu.roll(plane, (nz + i - 1) % nz, 1), lo)
        hi = jnp.where(lane1 == i, pltpu.roll(plane, (i + 2) % nz, 1), hi)
    fs[4] = lo
    fs[5] = hi
    faces = [(-1, 0, 0), (1, 0, 0), (0, -1, 0), (0, 1, 0), (0, 0, -1), (0, 0, 1)]
    faces = [(k, d) for k, d in enumerate(faces) if d in offsets]

    def fcopy(k, d):
        return pltpu.make_async_remote_copy(
            src_ref=fs.at[k], dst_ref=fr.at[k], send_sem=fsend.at[k], recv_sem=frecv.at[k],
            device_id=(mx + d[0], my + d[1], mz + d[2]), device_id_type=MESH)

    coarse_source(1, pr, vb)
    for k, d in faces:
        pl.when(exists(*d))(lambda k=k, d=d: fcopy(k, d).start())
    coarse_gather(1)
    coarse(1)
    for k, d in faces:
        back = opposite(d)

        @pl.when(exists(*back))
        def _(k=k, d=d):
            fcopy(k, d).wait_recv()
            if k == 0:
                vb[H + nx + 1, H : H + ny, 0:nz] = fr[0]
            if k == 1:
                vb[H - 2, H : H + ny, 0:nz] = fr[1]
            if k == 2:
                for i in range(nx):
                    vb[H + i, H + ny + 1 : H + ny + 2, 0:nz] = fr[2, i : i + 1]
            if k == 3:
                for i in range(nx):
                    vb[H + i, H - 2 : H - 1, 0:nz] = fr[3, i : i + 1]
            if k == 4:
                for i in range(nx):
                    old = vb[H + i, H : H + ny, nz : 2 * nz]
                    new = pltpu.roll(fr[4], (nz + 1 - i) % nz, 1)
                    vb[H + i, H : H + ny, nz : 2 * nz] = jnp.where(lane1 == 1, new, old)
            if k == 5:
                for i in range(nx):
                    old = vb[H + i, H : H + ny, nz : 2 * nz]
                    new = pltpu.roll(fr[5], (nz - 2 - i) % nz, 1)
                    vb[H + i, H : H + ny, nz : 2 * nz] = jnp.where(lane1 == nz - 2, new, old)

    correct(vb, H - 2, H + nx + 2)
    post(pr, vb, va, H - 1, H + nx + 1)

    def finish(p):
        c = va[p]
        out = KEEP * c + CB0 * pr[p] + CS * six(va, p, c)
        o_ref[p - H] = out[H : H + ny, 0:nz]

    loop(H, H + nx, finish)

    for d in offsets:
        @pl.when(exists(*d))
        def _(d=d):
            wcopy(d).wait_send()
    peers(lambda t, ax, ay, dz: gcopy(0, t, ax, ay, dz, me).wait_send())
    peers(lambda t, ax, ay, dz: gcopy(1, t, ax, ay, dz, me).wait_send())
    for k, d in faces:
        pl.when(exists(*d))(lambda k=k, d=d: fcopy(k, d).wait_send())


def body(counts, pressure, wind):
    gx, gy, gz = counts
    nx, ny, nz = pressure.shape
    cx, cy = nx // 2, ny // 2
    rx, ry, rz = nx + 2 * H, ny + 2 * H, 2 * nz
    group = gx * gy
    x1, tr, hy = gx * cx, gy * cy + 8, gy * cy // 2
    V = lambda *shape: pltpu.VMEM(shape, jnp.float32)
    D = lambda *shape: pltpu.SemaphoreType.DMA(shape)
    scratch = [
        V(rx, ry, rz), V(rx, ry, rz), V(rx, ry, rz),
        V(3, rx, ry, rz), V(3, rx, ry, rz), V(3, nx + 2 * HW, ry, rz),
        V(ry, rz), V(2, 9, ny, nz), V(2, 9, ny, nz), V(2, ny, nz), V(2, ny, nz),
        V(cx, ny, nz), V(cx * cy, nz),
        V(x1 + 2, tr, nz), V(x1 + 2, tr, nz), V(x1 + 2, tr, nz),
        V(x1 // 2 + 2, hy, nz), V(2, x1 // 2 + 2, hy, nz), V(x1 + 2, tr, nz),
        V(rx // 2, 2, ry, nz), V(rx // 2 * (ry // 2), nz), V(tr, nz),
        V(2, cx // 2, cy, nz), V(2, 2, cy, nz),
        V(2, group, cx // 2, cy, nz), V(2, group, 2, cy, nz),
        V(6, ny, nz), V(6, ny, nz),
        D(2), D(54), D(54), D(27), D(27), D(2, group, 3), D(2, group, 3), D(6), D(6),
    ]
    return pl.pallas_call(
        functools.partial(kernel, counts, (nx, ny, nz)),
        out_shape=jax.ShapeDtypeStruct(pressure.shape, jnp.float32),
        in_specs=[pl.BlockSpec(memory_space=pl.ANY)] * 2,
        out_specs=pl.BlockSpec(memory_space=pltpu.VMEM),
        scratch_shapes=scratch,
        compiler_params=pltpu.CompilerParams(collective_id=0, has_side_effects=True),
    )(pressure, wind)


def solution(mesh):
    counts = tuple(mesh.shape[name] for name in ("gx", "gy", "gz"))
    in_specs = (P("gx", "gy", "gz"), P(None, "gx", "gy", "gz"))
    return jax.shard_map(
        functools.partial(body, counts), mesh=mesh, in_specs=in_specs,
        out_specs=P("gx", "gy", "gz"), check_vma=False)
```
